8 devices in a mesh: fsdp: 8 (over z, y, x, core).
Axes of the slice: x: 2, y: 2, z: 1, core: 2. Of those that a mesh axis runs over, the one named last changes fastest.
Arguments:
- hidden: bfloat16 [48, 512, 1536], P('fsdp')
- grad_out: bfloat16 [48, 512, 1536], P('fsdp')
- positions: int32 [48, 512], P('fsdp')
- norm1_gain: bfloat16 [1536], P('fsdp')
- norm2_gain: bfloat16 [1536], P('fsdp')
- q_norm_gain: bfloat16 [128], replicated
- k_norm_gain: bfloat16 [128], replicated
- w_q: bfloat16 [1536, 1536], P('fsdp')
- w_k: bfloat16 [1536, 256], P('fsdp')
- w_v: bfloat16 [1536, 256], P('fsdp')
- w_o: bfloat16 [1536, 1536], P('fsdp')
- w_gate: bfloat16 [1536, 8960], P('fsdp')
- w_up: bfloat16 [1536, 8960], P('fsdp')
- w_down: bfloat16 [8960, 1536], P('fsdp')
Outputs:
- output 1: bfloat16 [48, 512, 1536], P('fsdp')
- output 2: bfloat16 [48, 512, 1536], P('fsdp')
- output 3: float32 [1536], P('fsdp')
- output 4: float32 [1536], P('fsdp')
- output 5: float32 [128], replicated
- output 6: float32 [128], replicated
- output 7: float32 [1536, 1536], P('fsdp')
- output 8: float32 [1536, 256], P('fsdp')
- output 9: float32 [1536, 256], P('fsdp')
- output 10: float32 [1536, 1536], P('fsdp')
- output 11: float32 [1536, 8960], P('fsdp')
- output 12: float32 [1536, 8960], P('fsdp')
- output 13: float32 [8960, 1536], P('fsdp')
All inputs are finite; a program needn't handle non-finite values.
Results may differ from the reference program's by a relative error of at most 0.02.
Values are sent between devices in bfloat16 or wider.
A program may use at most 1 GiB of HBM per device.

```python
import functools
import jax
import jax.numpy as jnp
from jax import lax

D = 1536
HEADS = 12
KV_HEADS = 2
HEAD = 128
FF = 8960
BATCH = 48
SEQ = 512
RMS_EPS = 1e-6
ROPE_THETA = 1000000.0
KV_GROUP = HEADS // KV_HEADS
TOKENS = BATCH * SEQ


def setup_inputs(seed: int = 0) -> dict:
    key_list = jax.random.split(jax.random.key(seed), 16)

    def normal_draw(key_index, arr_shape, std_scale):
        return (jax.random.normal(key_list[key_index], arr_shape, jnp.float32) * std_scale).astype(jnp.bfloat16)

    def gain_draw(key_index, arr_shape):
        return (1.0 + 0.3 * jax.random.normal(key_list[key_index], arr_shape, jnp.float32)).astype(jnp.bfloat16)

    start_key, stride_key = jax.random.split(key_list[2])
    start_pos = jax.random.randint(start_key, (BATCH, 1), 0, 4096)
    stride_pos = jax.random.randint(stride_key, (BATCH, SEQ), 1, 5)
    positions = (start_pos + jnp.cumsum(stride_pos, axis=1)).astype(jnp.int32)
    return {
        "hidden": normal_draw(0, (BATCH, SEQ, D), 1.0),
        "grad_out": normal_draw(1, (BATCH, SEQ, D), 1.0),
        "positions": positions,
        "norm1_gain": gain_draw(3, (D,)),
        "norm2_gain": gain_draw(4, (D,)),
        "q_norm_gain": gain_draw(5, (HEAD,)),
        "k_norm_gain": gain_draw(6, (HEAD,)),
        "w_q": normal_draw(7, (D, HEADS * HEAD), D ** -0.5),
        "w_k": normal_draw(8, (D, KV_HEADS * HEAD), D ** -0.5),
        "w_v": normal_draw(9, (D, KV_HEADS * HEAD), D ** -0.5),
        "w_o": normal_draw(10, (HEADS * HEAD, D), (HEADS * HEAD) ** -0.5),
        "w_gate": normal_draw(11, (D, FF), D ** -0.5),
        "w_up": normal_draw(12, (D, FF), D ** -0.5),
        "w_down": normal_draw(13, (FF, D), FF ** -0.5),
    }


def rms_scale(tensor):
    return lax.rsqrt(jnp.mean(tensor * tensor, axis=-1, keepdims=True) + RMS_EPS)


def rotate_half(tensor):
    half_dim = tensor.shape[-1] // 2
    return jnp.concatenate([-tensor[..., half_dim:], tensor[..., :half_dim]], axis=-1)


def attend_one(operands):
    q_seq, k_seq, v_seq = operands
    scores = jnp.einsum("skgd,tkd->kgst", q_seq.astype(jnp.float32), k_seq.astype(jnp.float32)) * (HEAD ** -0.5)
    causal = jnp.arange(SEQ)[:, None] >= jnp.arange(SEQ)[None, :]
    scores = jnp.where(causal, scores, -1e30)
    attn_probs = jax.nn.softmax(scores, axis=-1).astype(jnp.bfloat16)
    return jnp.einsum("kgst,tkd->skgd", attn_probs.astype(jnp.float32), v_seq.astype(jnp.float32)).astype(jnp.bfloat16)


def head_norm_rope(projected, num_heads, gain_vec, cos_t, sin_t):
    heads_float = projected.reshape(TOKENS, num_heads, HEAD).astype(jnp.float32)
    scaled = heads_float * rms_scale(heads_float) * gain_vec.astype(jnp.float32)
    return (scaled * cos_t + rotate_half(scaled) * sin_t).astype(jnp.bfloat16)


def layer_forward(positions, hidden, norm1_gain, norm2_gain, q_norm_gain, k_norm_gain, w_q, w_k, w_v, w_o, w_gate, w_up, w_down):
    x_float = hidden.reshape(TOKENS, D).astype(jnp.float32)
    normed = (x_float * rms_scale(x_float) * norm1_gain.astype(jnp.float32)).astype(jnp.bfloat16)
    q_proj = jnp.dot(normed, w_q, preferred_element_type=jnp.float32).astype(jnp.bfloat16)
    k_proj = jnp.dot(normed, w_k, preferred_element_type=jnp.float32).astype(jnp.bfloat16)
    v_proj = jnp.dot(normed, w_v, preferred_element_type=jnp.float32).astype(jnp.bfloat16)
    inv_freq = ROPE_THETA ** (-2.0 * jnp.arange(HEAD // 2, dtype=jnp.float32) / HEAD)
    rope_angle = positions.reshape(TOKENS, 1).astype(jnp.float32) * inv_freq
    cos_t = jnp.concatenate([jnp.cos(rope_angle), jnp.cos(rope_angle)], axis=-1)[:, None, :]
    sin_t = jnp.concatenate([jnp.sin(rope_angle), jnp.sin(rope_angle)], axis=-1)[:, None, :]
    q_rot = head_norm_rope(q_proj, HEADS, q_norm_gain, cos_t, sin_t)
    k_rot = head_norm_rope(k_proj, KV_HEADS, k_norm_gain, cos_t, sin_t)
    attn_ctx = lax.map(attend_one, (q_rot.reshape(BATCH, SEQ, KV_HEADS, KV_GROUP, HEAD), k_rot.reshape(BATCH, SEQ, KV_HEADS, HEAD), v_proj.reshape(BATCH, SEQ, KV_HEADS, HEAD)))
    attn_out = jnp.dot(attn_ctx.reshape(TOKENS, HEADS * HEAD), w_o, preferred_element_type=jnp.float32).astype(jnp.bfloat16)
    resid_float = (x_float + attn_out.astype(jnp.float32)).astype(jnp.bfloat16).astype(jnp.float32)
    mlp_in = (resid_float * rms_scale(resid_float) * norm2_gain.astype(jnp.float32)).astype(jnp.bfloat16)
    gate_proj = jnp.dot(mlp_in, w_gate, preferred_element_type=jnp.float32).astype(jnp.bfloat16)
    up_proj = jnp.dot(mlp_in, w_up, preferred_element_type=jnp.float32).astype(jnp.bfloat16)
    mlp_act = (jax.nn.silu(gate_proj.astype(jnp.float32)) * up_proj.astype(jnp.float32)).astype(jnp.bfloat16)
    down_proj = jnp.dot(mlp_act, w_down, preferred_element_type=jnp.float32).astype(jnp.bfloat16)
    layer_out = (resid_float + down_proj.astype(jnp.float32)).astype(jnp.bfloat16)
    return layer_out.reshape(BATCH, SEQ, D)


def mean_grad(grad_val):
    return grad_val.astype(jnp.float32) / TOKENS


def reference(hidden, grad_out, positions, norm1_gain, norm2_gain, q_norm_gain, k_norm_gain, w_q, w_k, w_v, w_o, w_gate, w_up, w_down):
    layer_out, pullback = jax.vjp(functools.partial(layer_forward, positions), hidden, norm1_gain, norm2_gain, q_norm_gain, k_norm_gain, w_q, w_k, w_v, w_o, w_gate, w_up, w_down)
    all_grads = pullback(grad_out)
    return (layer_out, all_grads[0].astype(jnp.bfloat16), mean_grad(all_grads[1]), mean_grad(all_grads[2]), mean_grad(all_grads[3]), mean_grad(all_grads[4]), mean_grad(all_grads[5]), mean_grad(all_grads[6]), mean_grad(all_grads[7]), mean_grad(all_grads[8]), mean_grad(all_grads[9]), mean_grad(all_grads[10]), mean_grad(all_grads[11]))
```

```python
import functools

import jax
import jax.numpy as jnp
from jax import lax
from jax.experimental import pallas as pl
from jax.experimental.pallas import tpu as pltpu
from jax.sharding import Mesh
from jax.sharding import PartitionSpec as P


RMS_EPS = 1e-6
ROPE_THETA = 1000000.0
F32 = jnp.float32
BF16 = jnp.bfloat16


def rms_scale(tensor):
    return lax.rsqrt(jnp.mean(tensor * tensor, axis=-1, keepdims=True) + RMS_EPS)


def norm_backward(d_unit, unit_val, scale_val):
    return scale_val * (d_unit - unit_val * jnp.mean(d_unit * unit_val, axis=-1, keepdims=True))


def matmul(left_op, right_op):
    return jnp.dot(left_op, right_op, preferred_element_type=F32)


def matmul_tn(left_op, right_op):
    return lax.dot_general(left_op, right_op, (((0,), (0,)), ((), ())), preferred_element_type=F32)


def matmul_nt(left_op, right_op):
    return lax.dot_general(left_op, right_op, (((1,), (1,)), ((), ())), preferred_element_type=F32)


def rope_tables(positions, head_dim):
    inv_freq = ROPE_THETA ** (-2.0 * jnp.arange(head_dim // 2, dtype=F32) / head_dim)
    rope_angle = positions.reshape(-1, 1).astype(F32) * inv_freq
    cos_half = jnp.cos(rope_angle)
    sin_half = jnp.sin(rope_angle)
    return jnp.concatenate([cos_half, cos_half], axis=-1), jnp.concatenate([-sin_half, sin_half], axis=-1)


def head_forward(projected, gain_vec, cos_t, sin_t):
    heads_float = projected.astype(F32)
    head_scale = rms_scale(heads_float)
    head_unit = heads_float * head_scale
    scaled = head_unit * gain_vec
    rotated = scaled * cos_t + pltpu.roll(scaled, scaled.shape[-1] // 2, 1) * sin_t
    return rotated.astype(BF16), head_unit, head_scale


def head_backward(d_rotated, head_unit, head_scale, gain_vec, cos_t, sin_t):
    d_scaled = d_rotated * cos_t - pltpu.roll(d_rotated, d_rotated.shape[-1] // 2, 1) * sin_t
    d_gain = jnp.sum(d_scaled * head_unit, axis=0, keepdims=True)
    return norm_backward(d_scaled * gain_vec, head_unit, head_scale).astype(BF16), d_gain


def probs_t(keys, queries, head_dim):
    key_len, q_len = keys.shape[0], queries.shape[0]
    scores = matmul_nt(keys, queries)
    tail = scores[key_len - q_len:]
    row = lax.broadcasted_iota(jnp.int32, tail.shape, 0)
    col = lax.broadcasted_iota(jnp.int32, tail.shape, 1)
    tail = jnp.where(row <= col, tail, -1e30)
    scores = tail if key_len == q_len else jnp.concatenate([scores[:key_len - q_len], tail], axis=0)
    top = jnp.max(scores, axis=0, keepdims=True)
    expo = jnp.exp((scores - top) * (head_dim ** -0.5))
    return expo * (1.0 / jnp.sum(expo, axis=0, keepdims=True))


def attention_forward_kernel(group, head_dim, q_tile, qkv_ref, cos_ref, sin_ref, qg_ref, kg_ref, ctx_ref):
    seq_len = qkv_ref.shape[0]
    cos_t, sin_t = cos_ref[...], sin_ref[...]
    base = group * head_dim
    k_rot, _, _ = head_forward(qkv_ref[:, base:base + head_dim], kg_ref[...], cos_t, sin_t)
    v_t = qkv_ref[:, base + head_dim:base + 2 * head_dim].T
    for head in range(group):
        lanes = slice(head * head_dim, (head + 1) * head_dim)
        q_rot, _, _ = head_forward(qkv_ref[:, lanes], qg_ref[...], cos_t, sin_t)
        for start in range(0, seq_len, q_tile):
            stop = start + q_tile
            probs = probs_t(k_rot[:stop], q_rot[start:stop], head_dim).astype(BF16)
            ctx_ref[start:stop, lanes] = matmul(v_t[:, :stop], probs).T.astype(BF16)


def attention_backward_kernel(group, head_dim, q_tile, qkv_ref, cos_ref, sin_ref, qg_ref, kg_ref, dctx_ref, dqkv_ref, gain_ref, dk_acc, dv_acc):
    seq_len = qkv_ref.shape[0]
    cos_t, sin_t = cos_ref[...], sin_ref[...]
    base = group * head_dim
    k_rot, k_unit, k_scale = head_forward(qkv_ref[:, base:base + head_dim], kg_ref[...], cos_t, sin_t)
    v_seq = qkv_ref[:, base + head_dim:base + 2 * head_dim]
    k_t = k_rot.T
    dk_acc[...] = jnp.zeros_like(dk_acc)
    dv_acc[...] = jnp.zeros_like(dv_acc)
    q_gain_sum = jnp.zeros((1, head_dim), F32)
    for head in range(group):
        lanes = slice(head * head_dim, (head + 1) * head_dim)
        q_rot, q_unit, q_scale = head_forward(qkv_ref[:, lanes], qg_ref[...], cos_t, sin_t)
        dq_tiles = []
        for start in range(0, seq_len, q_tile):
            stop = start + q_tile
            q_blk = q_rot[start:stop]
            d_out = dctx_ref[start:stop, lanes]
            probs = probs_t(k_rot[:stop], q_blk, head_dim)
            dv_acc[:stop, :] += matmul(probs.astype(BF16), d_out)
            d_probs = matmul_nt(v_seq[:stop], d_out)
            dot_row = jnp.sum(probs * d_probs, axis=0, keepdims=True)
            d_scores = (probs * (d_probs - dot_row) * (head_dim ** -0.5)).astype(BF16)
            dk_acc[:stop, :] += matmul(d_scores, q_blk)
            dq_tiles.append(matmul(k_t[:, :stop], d_scores).T)
        d_proj, d_gain = head_backward(jnp.concatenate(dq_tiles, axis=0), q_unit, q_scale, qg_ref[...], cos_t, sin_t)
        dqkv_ref[:, lanes] = d_proj
        q_gain_sum += d_gain
    d_proj, k_gain_sum = head_backward(dk_acc[...], k_unit, k_scale, kg_ref[...], cos_t, sin_t)
    dqkv_ref[:, base:base + head_dim] = d_proj
    dqkv_ref[:, base + head_dim:base + 2 * head_dim] = dv_acc[...].astype(BF16)

    @pl.when((pl.program_id(0) == 0) & (pl.program_id(1) == 0))
    def _():
        gain_ref[...] = jnp.zeros_like(gain_ref)

    gain_ref[0:1, :] += q_gain_sum
    gain_ref[1:2, :] += k_gain_sum


def norm_split_kernel(flag_ref, x_ref, attn_ref, gain_ref, resid_ref, scale_ref, norm_ref, own_ref, other_ref):
    resid = (x_ref[...].astype(F32) + attn_ref[...].astype(F32)).astype(BF16)
    resid_ref[...] = resid
    resid_float = resid.astype(F32)
    scale = rms_scale(resid_float)
    scale_ref[...] = jnp.broadcast_to(scale, scale_ref.shape)
    normed = (resid_float * scale * gain_ref[...]).astype(BF16)
    norm_ref[...] = normed
    first = flag_ref[0] == 0
    low = lax.broadcasted_iota(jnp.int32, (normed.shape[0], 128), 1) < 64
    for pair in range(normed.shape[1] // 768):
        tiles = [normed[:, pair * 768 + i * 128:pair * 768 + (i + 1) * 128].astype(F32) for i in range(6)]
        turned = [pltpu.roll(tile, 64, 1) for tile in tiles]
        even = [tiles[0], jnp.where(low, tiles[1], turned[3]), jnp.where(low, turned[3], turned[4])]
        odd = [jnp.where(low, turned[1], turned[2]), jnp.where(low, turned[2], tiles[4]), tiles[5]]
        for i in range(3):
            lanes = slice(pair * 384 + i * 128, pair * 384 + (i + 1) * 128)
            own_ref[:, lanes] = jnp.where(first, even[i], odd[i]).astype(BF16)
            other_ref[:, lanes] = jnp.where(first, odd[i], even[i]).astype(BF16)


def norm_split(core, x_flat, attn_out, gain, row_tile):
    tokens, width = x_flat.shape
    wide = pl.BlockSpec((row_tile, width), lambda i: (i, 0))
    half = pl.BlockSpec((row_tile, width // 2), lambda i: (i, 0))
    return pl.pallas_call(
        norm_split_kernel,
        out_shape=(
            jax.ShapeDtypeStruct((tokens, width), BF16),
            jax.ShapeDtypeStruct((tokens, 128), F32),
            jax.ShapeDtypeStruct((tokens, width), BF16),
            jax.ShapeDtypeStruct((tokens, width // 2), BF16),
            jax.ShapeDtypeStruct((tokens, width // 2), BF16),
        ),
        grid=(tokens // row_tile,),
        in_specs=[pl.BlockSpec(memory_space=pltpu.SMEM), wide, wide, pl.BlockSpec((1, width), lambda i: (0, 0))],
        out_specs=(wide, pl.BlockSpec((row_tile, 128), lambda i: (i, 0)), wide, half, half),
        compiler_params=pltpu.CompilerParams(dimension_semantics=("arbitrary",), vmem_limit_bytes=40 * 1024 * 1024),
        cost_estimate=pl.CostEstimate(flops=20 * tokens * width, bytes_accessed=10 * tokens * width, transcendentals=tokens),
        name="norm_split",
    )(core, x_flat, attn_out, gain)


def attention_specs(seq_len, group, head_dim):
    width = (group + 2) * head_dim
    return [
        pl.BlockSpec((seq_len, width), lambda b, k: (b, k)),
        pl.BlockSpec((seq_len, head_dim), lambda b, k: (b, 0)),
        pl.BlockSpec((seq_len, head_dim), lambda b, k: (b, 0)),
        pl.BlockSpec((1, head_dim), lambda b, k: (0, 0)),
        pl.BlockSpec((1, head_dim), lambda b, k: (0, 0)),
    ]


def attention_forward(qkv, cos_t, sin_t, q_gain, k_gain, batch, group, kv_heads, head_dim, q_tile):
    tokens = qkv.shape[0]
    seq_len = tokens // batch
    flops = 3 * tokens * seq_len * kv_heads * group * head_dim
    return pl.pallas_call(
        functools.partial(attention_forward_kernel, group, head_dim, q_tile),
        out_shape=jax.ShapeDtypeStruct((tokens, kv_heads * group * head_dim), BF16),
        grid=(batch, kv_heads),
        in_specs=attention_specs(seq_len, group, head_dim),
        out_specs=pl.BlockSpec((seq_len, group * head_dim), lambda b, k: (b, k)),
        compiler_params=pltpu.CompilerParams(dimension_semantics=("arbitrary", "arbitrary"), vmem_limit_bytes=40 * 1024 * 1024),
        cost_estimate=pl.CostEstimate(flops=flops, bytes_accessed=4 * qkv.size, transcendentals=tokens * seq_len * kv_heads * group),
        name="attn_fwd",
    )(qkv, cos_t, sin_t, q_gain, k_gain)


def attention_backward(qkv, cos_t, sin_t, q_gain, k_gain, d_ctx, batch, group, kv_heads, head_dim, q_tile):
    tokens = qkv.shape[0]
    seq_len = tokens // batch
    flops = 8 * tokens * seq_len * kv_heads * group * head_dim
    return pl.pallas_call(
        functools.partial(attention_backward_kernel, group, head_dim, q_tile),
        out_shape=(jax.ShapeDtypeStruct(qkv.shape, BF16), jax.ShapeDtypeStruct((8, head_dim), F32)),
        grid=(batch, kv_heads),
        in_specs=attention_specs(seq_len, group, head_dim) + [pl.BlockSpec((seq_len, group * head_dim), lambda b, k: (b, k))],
        out_specs=(pl.BlockSpec((seq_len, (group + 2) * head_dim), lambda b, k: (b, k)), pl.BlockSpec((8, head_dim), lambda b, k: (0, 0))),
        scratch_shapes=[pltpu.VMEM((seq_len, head_dim), F32)] * 2,
        compiler_params=pltpu.CompilerParams(dimension_semantics=("arbitrary", "arbitrary"), vmem_limit_bytes=40 * 1024 * 1024),
        cost_estimate=pl.CostEstimate(flops=flops, bytes_accessed=8 * qkv.size, transcendentals=tokens * seq_len * kv_heads * group),
        name="attn_bwd",
    )(qkv, cos_t, sin_t, q_gain, k_gain, d_ctx)


def solution(mesh):
    chips = mesh.devices.size // 2
    pair_mesh = Mesh(mesh.devices.reshape(chips, 2), ("chip", "core"))
    both = ("chip", "core")
    sharded = P(both)
    in_specs = (sharded, sharded, sharded, sharded, sharded, P(), P()) + (sharded,) * 7
    out_specs = (sharded, sharded, sharded, sharded, P(), P()) + (sharded,) * 7
    swap = [(0, 1), (1, 0)]

    def gather(shard):
        return lax.all_gather(shard, both, axis=0, tiled=True)

    def scatter(part, axes):
        return lax.psum_scatter(part, axes, scatter_dimension=0, tiled=True)

    def sum_all(values):
        values = values + lax.ppermute(values, "core", swap)
        step = 1
        while step < chips:
            values = values + lax.ppermute(values, "chip", [(c, c ^ step) for c in range(chips)])
            step *= 2
        return values

    def device_step(hidden, grad_out, positions, norm1_gain, norm2_gain, q_norm_gain, k_norm_gain, w_q, w_k, w_v, w_o, w_gate, w_up, w_down):
        batch, seq_len, width = hidden.shape
        head_dim = q_norm_gain.shape[0]
        kv_heads = w_k.shape[1] // head_dim
        group = w_q.shape[1] // head_dim // kv_heads
        tokens = batch * seq_len
        rows = w_q.shape[0]
        core = lax.axis_index("core")
        first = core == 0
        device = lax.axis_index("chip") * 2 + core
        inv_tokens = 1.0 / (tokens * chips * 2)
        q_tile = 256

        def own(even, odd):
            return jnp.where(first, even, odd)

        pieces = []
        for head in range(kv_heads):
            pieces.append(w_q[:, head * group * head_dim:(head + 1) * group * head_dim])
            pieces.append(w_k[:, head * head_dim:(head + 1) * head_dim])
            pieces.append(w_v[:, head * head_dim:(head + 1) * head_dim])
        qkv_width = kv_heads * (group + 2) * head_dim
        pieces.append(jnp.pad(jnp.stack([norm1_gain, norm2_gain], axis=1), ((0, 0), (0, head_dim - 2))))
        qkv_full = gather(jnp.concatenate(pieces, axis=1))
        wo_full = gather(w_o)
        gate_full = gather(w_gate)
        up_full = gather(w_up)
        down_full = gather(w_down)
        w_qkv = qkv_full[:, :qkv_width]
        gain1 = qkv_full[:, qkv_width].astype(F32)
        gain2 = qkv_full[:, qkv_width + 1].astype(F32)
        q_gain = q_norm_gain.astype(F32).reshape(1, head_dim)
        k_gain = k_norm_gain.astype(F32).reshape(1, head_dim)

        x_float = hidden.reshape(tokens, width).astype(F32)
        dy = grad_out.reshape(tokens, width)
        x_scale = rms_scale(x_float)
        normed = (x_float * x_scale * gain1).astype(BF16)
        qkv = matmul(normed, w_qkv).astype(BF16)
        cos_t, sin_t = rope_tables(positions, head_dim)
        ctx = attention_forward(qkv, cos_t, sin_t, q_gain, k_gain, batch, group, kv_heads, head_dim, q_tile)
        attn_out = matmul(ctx, wo_full).astype(BF16)
        resid, r_wide, mlp_in, in_own, in_other = norm_split(core.reshape(1), hidden.reshape(tokens, width), attn_out, gain2.reshape(1, width), 256)
        resid_float = resid.astype(F32)
        r_scale = r_wide[:, :1]
        gate_proj = matmul(mlp_in, gate_full).astype(BF16)
        up_proj = matmul(mlp_in, up_full).astype(BF16)
        mlp_act = (jax.nn.silu(gate_proj.astype(F32)) * up_proj.astype(F32)).astype(BF16)

        half = width // 2
        dy_own, dy_other = own(dy[:, :half], dy[:, half:]), own(dy[:, half:], dy[:, :half])
        down_recv = lax.ppermute(matmul_tn(mlp_act, dy_other), "core", swap)
        down_proj = matmul(mlp_act, down_full).astype(BF16)
        layer_out = (resid_float + down_proj.astype(F32)).astype(BF16)
        dy_own, layer_out = lax.optimization_barrier((dy_own, layer_out))
        down_pair = (matmul_tn(mlp_act, dy_own) + down_recv) * inv_tokens
        down_rows = scatter(down_pair, "chip")
        drows = down_rows.shape[0] // 2
        down_back = lax.ppermute(own(down_rows[drows:], down_rows[:drows]), "core", swap)
        down_mine = own(down_rows[:drows], down_rows[drows:])
        g_down = own(jnp.concatenate([down_mine, down_back], axis=1), jnp.concatenate([down_back, down_mine], axis=1))

        dy_late, layer_out, _ = lax.optimization_barrier((dy, layer_out, down_pair))
        d_mlp_act = matmul_nt(dy_late, down_full)
        gate_float = gate_proj.astype(F32)
        gate_sig = jax.nn.sigmoid(gate_float)
        d_up = (d_mlp_act * gate_float * gate_sig).astype(BF16)
        d_gate = (d_mlp_act * up_proj.astype(F32) * gate_sig * (1.0 + gate_float * (1.0 - gate_sig))).astype(BF16)

        gate_recv = lax.ppermute(matmul_tn(in_other, d_gate), "core", swap)
        up_recv = lax.ppermute(matmul_tn(in_other, d_up), "core", swap)
        gate_pair = (matmul_tn(in_own, d_gate) + gate_recv) * inv_tokens
        up_pair = (matmul_tn(in_own, d_up) + up_recv) * inv_tokens
        g_gate = scatter(gate_pair, "chip")
        g_up = scatter(up_pair, "chip")
        d_gate, d_up, _, _ = lax.optimization_barrier((d_gate, d_up, gate_pair, up_pair))

        d_mlp_in = matmul_nt(d_gate, gate_full) + matmul_nt(d_up, up_full)
        r_unit = resid_float * r_scale
        grad_norm2 = jnp.sum(d_mlp_in * r_unit, axis=0)
        d_resid = dy.astype(F32) + norm_backward(d_mlp_in * gain2, r_unit, r_scale)
        d_resid_bf = d_resid.astype(BF16)
        wo_part = matmul_tn(ctx, d_resid_bf) * inv_tokens
        g_wo = scatter(wo_part, both)
        d_resid_bf, _ = lax.optimization_barrier((d_resid_bf, wo_part))
        d_ctx = matmul_nt(d_resid_bf, wo_full).astype(BF16)
        d_qkv, gain_sums = attention_backward(qkv, cos_t, sin_t, q_gain, k_gain, d_ctx, batch, group, kv_heads, head_dim, q_tile)
        g_qkv = scatter(matmul_tn(normed, d_qkv) * inv_tokens, both)

        d_normed = matmul_nt(d_qkv, w_qkv)
        x_unit = x_float * x_scale
        grad_norm1 = jnp.sum(d_normed * x_unit, axis=0)
        d_hidden = (d_resid + norm_backward(d_normed * gain1, x_unit, x_scale)).astype(BF16)

        small = jnp.concatenate([grad_norm1, grad_norm2, gain_sums[0], gain_sums[1]]) * inv_tokens
        small = sum_all(small.reshape(-1, 128)).reshape(-1)
        g_norm1 = lax.dynamic_slice_in_dim(small[:width], device * rows, rows)
        g_norm2 = lax.dynamic_slice_in_dim(small[width:2 * width], device * rows, rows)
        g_qgain = small[2 * width:2 * width + head_dim]
        g_kgain = small[2 * width + head_dim:]

        qs, ks, vs = [], [], []
        for head in range(kv_heads):
            start = head * (group + 2) * head_dim
            qs.append(g_qkv[:, start:start + group * head_dim])
            ks.append(g_qkv[:, start + group * head_dim:start + (group + 1) * head_dim])
            vs.append(g_qkv[:, start + (group + 1) * head_dim:start + (group + 2) * head_dim])
        g_wq, g_wk, g_wv = (jnp.concatenate(part, axis=1) for part in (qs, ks, vs))
        return (layer_out.reshape(hidden.shape), d_hidden.reshape(hidden.shape), g_norm1, g_norm2, g_qgain, g_kgain, g_wq, g_wk, g_wv, g_wo, g_gate, g_up, g_down)

    return jax.shard_map(device_step, mesh=pair_mesh, in_specs=in_specs, out_specs=out_specs, check_vma=False)
```

```python
import functools

import jax
import jax.numpy as jnp
from jax import lax
from jax.experimental import pallas as pl
from jax.experimental.pallas import tpu as pltpu
from jax.sharding import Mesh
from jax.sharding import PartitionSpec as P


RMS_EPS = 1e-6
ROPE_THETA = 1000000.0
LOG2_E = 1.4426950408889634
F32 = jnp.float32
BF16 = jnp.bfloat16


def rms_scale(tensor):
    return lax.rsqrt(jnp.mean(tensor * tensor, axis=-1, keepdims=True) + RMS_EPS)


def norm_backward(d_unit, unit_val, scale_val):
    return scale_val * (d_unit - unit_val * jnp.mean(d_unit * unit_val, axis=-1, keepdims=True))


def matmul(left_op, right_op):
    return jnp.dot(left_op, right_op, preferred_element_type=F32)


def matmul_tn(left_op, right_op):
    return lax.dot_general(left_op, right_op, (((0,), (0,)), ((), ())), preferred_element_type=F32)


def matmul_nt(left_op, right_op):
    return lax.dot_general(left_op, right_op, (((1,), (1,)), ((), ())), preferred_element_type=F32)


def rope_tables(positions, head_dim):
    inv_freq = ROPE_THETA ** (-2.0 * jnp.arange(head_dim // 2, dtype=F32) / head_dim)
    rope_angle = positions.reshape(-1, 1).astype(F32) * inv_freq
    cos_half = jnp.cos(rope_angle)
    sin_half = jnp.sin(rope_angle)
    return jnp.concatenate([cos_half, cos_half], axis=-1), jnp.concatenate([-sin_half, sin_half], axis=-1)


def head_forward(projected, gain_vec, cos_t, sin_t):
    heads_float = projected.astype(F32)
    head_scale = rms_scale(heads_float)
    head_unit = heads_float * head_scale
    scaled = head_unit * gain_vec
    rotated = scaled * cos_t + pltpu.roll(scaled, scaled.shape[-1] // 2, 1) * sin_t
    return rotated.astype(BF16), head_unit, head_scale


def head_backward(d_rotated, head_unit, head_scale, gain_vec, cos_t, sin_t):
    d_scaled = d_rotated * cos_t - pltpu.roll(d_rotated, d_rotated.shape[-1] // 2, 1) * sin_t
    d_gain = jnp.sum(d_scaled * head_unit, axis=0, keepdims=True)
    return norm_backward(d_scaled * gain_vec, head_unit, head_scale).astype(BF16), d_gain


def probs_t(keys, queries, head_dim):
    key_len, q_len = keys.shape[0], queries.shape[0]
    scores = matmul_nt(keys, queries)
    tail = scores[key_len - q_len:]
    row = lax.broadcasted_iota(jnp.int32, tail.shape, 0)
    col = lax.broadcasted_iota(jnp.int32, tail.shape, 1)
    tail = jnp.where(row <= col, tail, -1e30)
    scores = tail if key_len == q_len else jnp.concatenate([scores[:key_len - q_len], tail], axis=0)
    top = jnp.max(scores, axis=0, keepdims=True)
    expo = jnp.exp2((scores - top) * (head_dim ** -0.5 * LOG2_E))
    return expo * (1.0 / jnp.sum(expo, axis=0, keepdims=True))


def attention_forward_kernel(group, head_dim, q_tile, qkv_ref, cos_ref, sin_ref, qg_ref, kg_ref, ctx_ref):
    seq_len = qkv_ref.shape[0]
    cos_t, sin_t = cos_ref[...], sin_ref[...]
    base = group * head_dim
    k_rot, _, _ = head_forward(qkv_ref[:, base:base + head_dim], kg_ref[...], cos_t, sin_t)
    v_t = qkv_ref[:, base + head_dim:base + 2 * head_dim].T
    for head in range(group):
        lanes = slice(head * head_dim, (head + 1) * head_dim)
        q_rot, _, _ = head_forward(qkv_ref[:, lanes], qg_ref[...], cos_t, sin_t)
        for start in range(0, seq_len, q_tile):
            stop = start + q_tile
            probs = probs_t(k_rot[:stop], q_rot[start:stop], head_dim).astype(BF16)
            ctx_ref[start:stop, lanes] = matmul(v_t[:, :stop], probs).T.astype(BF16)


def attention_backward_kernel(group, head_dim, q_tile, qkv_ref, cos_ref, sin_ref, qg_ref, kg_ref, dctx_ref, dqkv_ref, gain_ref, dk_acc, dv_acc):
    seq_len = qkv_ref.shape[0]
    cos_t, sin_t = cos_ref[...], sin_ref[...]
    base = group * head_dim
    k_rot, k_unit, k_scale = head_forward(qkv_ref[:, base:base + head_dim], kg_ref[...], cos_t, sin_t)
    v_seq = qkv_ref[:, base + head_dim:base + 2 * head_dim]
    k_t = k_rot.T
    dk_acc[...] = jnp.zeros_like(dk_acc)
    dv_acc[...] = jnp.zeros_like(dv_acc)
    q_gain_sum = jnp.zeros((1, head_dim), F32)
    for head in range(group):
        lanes = slice(head * head_dim, (head + 1) * head_dim)
        q_rot, q_unit, q_scale = head_forward(qkv_ref[:, lanes], qg_ref[...], cos_t, sin_t)
        dq_tiles = []
        for start in range(0, seq_len, q_tile):
            stop = start + q_tile
            q_blk = q_rot[start:stop]
            d_out = dctx_ref[start:stop, lanes]
            probs = probs_t(k_rot[:stop], q_blk, head_dim)
            dv_acc[:stop, :] += matmul(probs.astype(BF16), d_out)
            d_probs = matmul_nt(v_seq[:stop], d_out)
            dot_row = jnp.sum(probs * d_probs, axis=0, keepdims=True)
            d_scores = (probs * (d_probs - dot_row)).astype(BF16)
            dk_acc[:stop, :] += matmul(d_scores, q_blk)
            dq_tiles.append(matmul(k_t[:, :stop], d_scores).T)
        d_proj, d_gain = head_backward(jnp.concatenate(dq_tiles, axis=0) * (head_dim ** -0.5), q_unit, q_scale, qg_ref[...], cos_t, sin_t)
        dqkv_ref[:, lanes] = d_proj
        q_gain_sum += d_gain
    d_proj, k_gain_sum = head_backward(dk_acc[...] * (head_dim ** -0.5), k_unit, k_scale, kg_ref[...], cos_t, sin_t)
    dqkv_ref[:, base:base + head_dim] = d_proj
    dqkv_ref[:, base + head_dim:base + 2 * head_dim] = dv_acc[...].astype(BF16)

    @pl.when((pl.program_id(0) == 0) & (pl.program_id(1) == 0))
    def _():
        gain_ref[...] = jnp.zeros_like(gain_ref)

    gain_ref[0:1, :] += q_gain_sum
    gain_ref[1:2, :] += k_gain_sum


def norm_split_kernel(flag_ref, x_ref, attn_ref, gain_ref, resid_ref, scale_ref, norm_ref, own_ref, other_ref):
    resid = (x_ref[...].astype(F32) + attn_ref[...].astype(F32)).astype(BF16)
    resid_ref[...] = resid
    resid_float = resid.astype(F32)
    scale = rms_scale(resid_float)
    scale_ref[...] = jnp.broadcast_to(scale, scale_ref.shape)
    normed = (resid_float * scale * gain_ref[...]).astype(BF16)
    norm_ref[...] = normed
    first = flag_ref[0] == 0
    low = lax.broadcasted_iota(jnp.int32, (normed.shape[0], 128), 1) < 64
    for pair in range(normed.shape[1] // 768):
        tiles = [normed[:, pair * 768 + i * 128:pair * 768 + (i + 1) * 128].astype(F32) for i in range(6)]
        turned = [pltpu.roll(tile, 64, 1) for tile in tiles]
        even = [tiles[0], jnp.where(low, tiles[1], turned[3]), jnp.where(low, turned[3], turned[4])]
        odd = [jnp.where(low, turned[1], turned[2]), jnp.where(low, turned[2], tiles[4]), tiles[5]]
        for i in range(3):
            lanes = slice(pair * 384 + i * 128, pair * 384 + (i + 1) * 128)
            own_ref[:, lanes] = jnp.where(first, even[i], odd[i]).astype(BF16)
            other_ref[:, lanes] = jnp.where(first, odd[i], even[i]).astype(BF16)


def norm_split(core, x_flat, attn_out, gain, row_tile):
    tokens, width = x_flat.shape
    wide = pl.BlockSpec((row_tile, width), lambda i: (i, 0))
    half = pl.BlockSpec((row_tile, width // 2), lambda i: (i, 0))
    return pl.pallas_call(
        norm_split_kernel,
        out_shape=(
            jax.ShapeDtypeStruct((tokens, width), BF16),
            jax.ShapeDtypeStruct((tokens, 128), F32),
            jax.ShapeDtypeStruct((tokens, width), BF16),
            jax.ShapeDtypeStruct((tokens, width // 2), BF16),
            jax.ShapeDtypeStruct((tokens, width // 2), BF16),
        ),
        grid=(tokens // row_tile,),
        in_specs=[pl.BlockSpec(memory_space=pltpu.SMEM), wide, wide, pl.BlockSpec((1, width), lambda i: (0, 0))],
        out_specs=(wide, pl.BlockSpec((row_tile, 128), lambda i: (i, 0)), wide, half, half),
        compiler_params=pltpu.CompilerParams(dimension_semantics=("arbitrary",), vmem_limit_bytes=40 * 1024 * 1024),
        cost_estimate=pl.CostEstimate(flops=20 * tokens * width, bytes_accessed=10 * tokens * width, transcendentals=tokens),
        name="norm_split",
    )(core, x_flat, attn_out, gain)


def attention_specs(seq_len, group, head_dim):
    width = (group + 2) * head_dim
    return [
        pl.BlockSpec((seq_len, width), lambda b, k: (b, k)),
        pl.BlockSpec((seq_len, head_dim), lambda b, k: (b, 0)),
        pl.BlockSpec((seq_len, head_dim), lambda b, k: (b, 0)),
        pl.BlockSpec((1, head_dim), lambda b, k: (0, 0)),
        pl.BlockSpec((1, head_dim), lambda b, k: (0, 0)),
    ]


def attention_forward(qkv, cos_t, sin_t, q_gain, k_gain, batch, group, kv_heads, head_dim, q_tile):
    tokens = qkv.shape[0]
    seq_len = tokens // batch
    flops = 3 * tokens * seq_len * kv_heads * group * head_dim
    return pl.pallas_call(
        functools.partial(attention_forward_kernel, group, head_dim, q_tile),
        out_shape=jax.ShapeDtypeStruct((tokens, kv_heads * group * head_dim), BF16),
        grid=(batch, kv_heads),
        in_specs=attention_specs(seq_len, group, head_dim),
        out_specs=pl.BlockSpec((seq_len, group * head_dim), lambda b, k: (b, k)),
        compiler_params=pltpu.CompilerParams(dimension_semantics=("arbitrary", "arbitrary"), vmem_limit_bytes=40 * 1024 * 1024),
        cost_estimate=pl.CostEstimate(flops=flops, bytes_accessed=4 * qkv.size, transcendentals=tokens * seq_len * kv_heads * group),
        name="attn_fwd",
    )(qkv, cos_t, sin_t, q_gain, k_gain)


def attention_backward(qkv, cos_t, sin_t, q_gain, k_gain, d_ctx, batch, group, kv_heads, head_dim, q_tile):
    tokens = qkv.shape[0]
    seq_len = tokens // batch
    flops = 8 * tokens * seq_len * kv_heads * group * head_dim
    return pl.pallas_call(
        functools.partial(attention_backward_kernel, group, head_dim, q_tile),
        out_shape=(jax.ShapeDtypeStruct(qkv.shape, BF16), jax.ShapeDtypeStruct((8, head_dim), F32)),
        grid=(batch, kv_heads),
        in_specs=attention_specs(seq_len, group, head_dim) + [pl.BlockSpec((seq_len, group * head_dim), lambda b, k: (b, k))],
        out_specs=(pl.BlockSpec((seq_len, (group + 2) * head_dim), lambda b, k: (b, k)), pl.BlockSpec((8, head_dim), lambda b, k: (0, 0))),
        scratch_shapes=[pltpu.VMEM((seq_len, head_dim), F32)] * 2,
        compiler_params=pltpu.CompilerParams(dimension_semantics=("arbitrary", "arbitrary"), vmem_limit_bytes=40 * 1024 * 1024),
        cost_estimate=pl.CostEstimate(flops=flops, bytes_accessed=8 * qkv.size, transcendentals=tokens * seq_len * kv_heads * group),
        name="attn_bwd",
    )(qkv, cos_t, sin_t, q_gain, k_gain, d_ctx)


def solution(mesh):
    chips = mesh.devices.size // 2
    pair_mesh = Mesh(mesh.devices.reshape(chips, 2), ("chip", "core"))
    both = ("chip", "core")
    sharded = P(both)
    in_specs = (sharded, sharded, sharded, sharded, sharded, P(), P()) + (sharded,) * 7
    out_specs = (sharded, sharded, sharded, sharded, P(), P()) + (sharded,) * 7
    swap = [(0, 1), (1, 0)]

    def gather(shard, axes=both):
        return lax.all_gather(shard, axes, axis=0, tiled=True)

    def scatter(part, axes):
        return lax.psum_scatter(part, axes, scatter_dimension=0, tiled=True)

    def sum_all(values):
        values = values + lax.ppermute(values, "core", swap)
        step = 1
        while step < chips:
            values = values + lax.ppermute(values, "chip", [(c, c ^ step) for c in range(chips)])
            step *= 2
        return values

    def device_step(hidden, grad_out, positions, norm1_gain, norm2_gain, q_norm_gain, k_norm_gain, w_q, w_k, w_v, w_o, w_gate, w_up, w_down):
        batch, seq_len, width = hidden.shape
        head_dim = q_norm_gain.shape[0]
        kv_heads = w_k.shape[1] // head_dim
        group = w_q.shape[1] // head_dim // kv_heads
        tokens = batch * seq_len
        rows = w_q.shape[0]
        core = lax.axis_index("core")
        first = core == 0
        device = lax.axis_index("chip") * 2 + core
        inv_tokens = 1.0 / (tokens * chips * 2)
        q_tile = 256

        def own(even, odd):
            return jnp.where(first, even, odd)

        pieces = []
        for head in range(kv_heads):
            pieces.append(w_q[:, head * group * head_dim:(head + 1) * group * head_dim])
            pieces.append(w_k[:, head * head_dim:(head + 1) * head_dim])
            pieces.append(w_v[:, head * head_dim:(head + 1) * head_dim])
        qkv_width = kv_heads * (group + 2) * head_dim
        pieces.append(jnp.pad(jnp.stack([norm1_gain, norm2_gain], axis=1), ((0, 0), (0, head_dim - 2))))
        qkv_full = gather(jnp.concatenate(pieces, axis=1))
        wo_full = gather(w_o)
        block = w_down.shape[0]
        chunk = block * chips

        def columns(weight, k):
            return jnp.concatenate([weight[:, (2 * c + k) * block:(2 * c + k + 1) * block] for c in range(chips)], axis=1)

        gate_w, up_w = [], []
        for k in range(2):
            gate_w.append(gather(columns(w_gate, k)))
            up_w.append(gather(columns(w_up, k)))
        down_full = gather(w_down, ("core", "chip"))
        down_w = [down_full[:chunk], down_full[chunk:]]
        w_qkv = qkv_full[:, :qkv_width]
        gain1 = qkv_full[:, qkv_width].astype(F32)
        gain2 = qkv_full[:, qkv_width + 1].astype(F32)
        q_gain = q_norm_gain.astype(F32).reshape(1, head_dim)
        k_gain = k_norm_gain.astype(F32).reshape(1, head_dim)

        x_float = hidden.reshape(tokens, width).astype(F32)
        dy = grad_out.reshape(tokens, width)
        x_scale = rms_scale(x_float)
        normed = (x_float * x_scale * gain1).astype(BF16)
        qkv = matmul(normed, w_qkv).astype(BF16)
        cos_t, sin_t = rope_tables(positions, head_dim)
        ctx = attention_forward(qkv, cos_t, sin_t, q_gain, k_gain, batch, group, kv_heads, head_dim, q_tile)
        attn_out = matmul(ctx, wo_full).astype(BF16)
        resid, r_wide, mlp_in, in_own, in_other = norm_split(core.reshape(1), hidden.reshape(tokens, width), attn_out, gain2.reshape(1, width), 256)
        resid_float = resid.astype(F32)
        r_scale = r_wide[:, :1]
        gate_proj, up_proj, mlp_act = [], [], []
        for k in range(2):
            gate_proj.append(matmul(mlp_in, gate_w[k]).astype(BF16))
            up_proj.append(matmul(mlp_in, up_w[k]).astype(BF16))
            mlp_act.append((jax.nn.silu(gate_proj[k].astype(F32)) * up_proj[k].astype(F32)).astype(BF16))

        half = width // 2
        dy_own, dy_other = own(dy[:, :half], dy[:, half:]), own(dy[:, half:], dy[:, :half])
        down_recv = [lax.ppermute(matmul_tn(mlp_act[k], dy_other), "core", swap) for k in range(2)]
        dy_own, _ = lax.optimization_barrier((dy_own, mlp_act[1]))
        down_pair = [(matmul_tn(mlp_act[k], dy_own) + down_recv[k]) * inv_tokens for k in range(2)]
        down_rows = [scatter(down_pair[k], "chip") for k in range(2)]
        down_back = lax.ppermute(own(down_rows[1], down_rows[0]), "core", swap)
        down_mine = own(down_rows[0], down_rows[1])
        g_down = own(jnp.concatenate([down_mine, down_back], axis=1), jnp.concatenate([down_back, down_mine], axis=1))

        held = tuple(down_pair)
        dy_late = dy
        d_gate, d_up, gate_rows, up_rows = [], [], [], []
        for k in range(2):
            dy_late = lax.optimization_barrier((dy_late,) + held)[0]
            d_mlp_act = matmul_nt(dy_late, down_w[k])
            gate_float = gate_proj[k].astype(F32)
            gate_sig = jax.nn.sigmoid(gate_float)
            d_up.append((d_mlp_act * gate_float * gate_sig).astype(BF16))
            d_gate.append((d_mlp_act * up_proj[k].astype(F32) * gate_sig * (1.0 + gate_float * (1.0 - gate_sig))).astype(BF16))
            gate_recv = lax.ppermute(matmul_tn(in_other, d_gate[k]), "core", swap)
            up_recv = lax.ppermute(matmul_tn(in_other, d_up[k]), "core", swap)
            gate_pair = (matmul_tn(in_own, d_gate[k]) + gate_recv) * inv_tokens
            up_pair = (matmul_tn(in_own, d_up[k]) + up_recv) * inv_tokens
            gate_rows.append(scatter(gate_pair, "chip"))
            up_rows.append(scatter(up_pair, "chip"))
            held = (gate_pair, up_pair)

        def interleave(parts):
            return jnp.concatenate([parts[i % 2][:, (i // 2) * block:(i // 2 + 1) * block] for i in range(2 * chips)], axis=1)

        g_gate, g_up = interleave(gate_rows), interleave(up_rows)
        late = lax.optimization_barrier((d_gate[0], d_up[0], d_gate[1], d_up[1]) + held)
        d_mlp_in = matmul_nt(late[0], gate_w[0]) + matmul_nt(late[1], up_w[0]) + matmul_nt(late[2], gate_w[1]) + matmul_nt(late[3], up_w[1])
        r_unit = resid_float * r_scale
        grad_norm2 = jnp.sum(d_mlp_in * r_unit, axis=0)
        d_resid = dy.astype(F32) + norm_backward(d_mlp_in * gain2, r_unit, r_scale)
        d_resid_bf = d_resid.astype(BF16)
        wo_part = matmul_tn(ctx, d_resid_bf) * inv_tokens
        g_wo = scatter(wo_part, both)
        d_resid_bf, _ = lax.optimization_barrier((d_resid_bf, wo_part))
        d_ctx = matmul_nt(d_resid_bf, wo_full).astype(BF16)
        d_qkv, gain_sums = attention_backward(qkv, cos_t, sin_t, q_gain, k_gain, d_ctx, batch, group, kv_heads, head_dim, q_tile)
        qkv_part = matmul_tn(normed, d_qkv) * inv_tokens
        g_qkv = scatter(qkv_part, both)

        d_normed = matmul_nt(d_qkv, w_qkv)
        x_unit = x_float * x_scale
        grad_norm1 = jnp.sum(d_normed * x_unit, axis=0)
        d_hidden = (d_resid + norm_backward(d_normed * gain1, x_unit, x_scale)).astype(BF16)

        act0, act1, d_hidden, _ = lax.optimization_barrier((mlp_act[0], mlp_act[1], d_hidden, qkv_part))
        down_proj = (matmul(act0, down_w[0]) + matmul(act1, down_w[1])).astype(BF16)
        layer_out = (resid_float + down_proj.astype(F32)).astype(BF16)

        small = jnp.concatenate([grad_norm1, grad_norm2, gain_sums[0], gain_sums[1]]) * inv_tokens
        small = sum_all(small.reshape(-1, 128)).reshape(-1)
        g_norm1 = lax.dynamic_slice_in_dim(small[:width], device * rows, rows)
        g_norm2 = lax.dynamic_slice_in_dim(small[width:2 * width], device * rows, rows)
        g_qgain = small[2 * width:2 * width + head_dim]
        g_kgain = small[2 * width + head_dim:]

        qs, ks, vs = [], [], []
        for head in range(kv_heads):
            start = head * (group + 2) * head_dim
            qs.append(g_qkv[:, start:start + group * head_dim])
            ks.append(g_qkv[:, start + group * head_dim:start + (group + 1) * head_dim])
            vs.append(g_qkv[:, start + (group + 1) * head_dim:start + (group + 2) * head_dim])
        g_wq, g_wk, g_wv = (jnp.concatenate(part, axis=1) for part in (qs, ks, vs))
        return (layer_out.reshape(hidden.shape), d_hidden.reshape(hidden.shape), g_norm1, g_norm2, g_qgain, g_kgain, g_wq, g_wk, g_wv, g_wo, g_gate, g_up, g_down)

    return jax.shard_map(device_step, mesh=pair_mesh, in_specs=in_specs, out_specs=out_specs, check_vma=False)
```
